32 devices in a mesh: row: 4 (over z), col: 8 (over y, x, core).
Axes of the slice: x: 2, y: 2, z: 4, core: 2. Of those that a mesh axis runs over, the one named last changes fastest.
Arguments:
- momentum: float32 [8192, 26624], P('row', 'col'), may hold values from -6 to 6
- gradient: bfloat16 [8192, 26624], P('row', 'col'), may hold values from -150 to 150
- q_basis: bfloat16 [26624, 512], P('col', 'row'), may hold values from -0.0390625 to 0.0390625
Outputs:
- momentum_next: float32 [8192, 26624], P('row', 'col')
- p_basis: float32 [8192, 512], P(('row', 'col'))
- q_next: float32 [26624, 512], P('col', 'row')
The draws below stay inside these ranges and needn't reach their ends.
All inputs are finite; a program needn't handle non-finite values.
Results may differ from the reference program's by a relative error of at most 0.0065.
Values may be sent and summed in bfloat16 or wider, within the bound.
No kernel may reach another device: no remote copies, remote signals or barrier semaphores. Data moves between devices by JAX's collectives and lax.ppermute only.
A program may use at most 128 MiB of HBM per device.

```python
import math
import jax
import jax.numpy as jnp
from jax import lax

ROWS = 8192
COLS = 26624
RANK = 512


def draw_gradient(key, part):
    base_key = jax.random.fold_in(key, 17)
    streams = jax.random.split(base_key, 6)
    signal_rank = RANK // 2
    row_ramp = jnp.exp(math.log(3.0) * jnp.arange(ROWS, dtype=jnp.float32) / ROWS)
    col_ramp = jnp.exp(math.log(3.0) * jnp.arange(COLS, dtype=jnp.float32) / COLS)
    values = jax.random.truncated_normal(streams[0], -4.0, 4.0, (ROWS, COLS), jnp.float32)
    row_rough = jnp.exp(jax.random.uniform(streams[1], (ROWS,), jnp.float32, 0.0, math.log(2.0)))
    col_rough = jnp.exp(jax.random.uniform(streams[2], (COLS,), jnp.float32, 0.0, math.log(2.0)))
    target = 6.0
    strengths = jnp.exp(jax.random.uniform(streams[3], (signal_rank,), jnp.float32, 0.0, math.log(4.0)))
    left_factor = jax.random.normal(streams[4], (ROWS, signal_rank), jnp.float32)
    right_factor = jax.random.normal(streams[5], (COLS, signal_rank), jnp.float32)
    weighting = target / 3.64 * strengths / jnp.sqrt(jnp.sum(strengths * strengths))
    signal = jnp.dot(left_factor * weighting[None, :], right_factor.T, precision=lax.Precision.HIGHEST)
    noise = 0.25 * values * (row_ramp * row_rough)[:, None] * (col_ramp * col_rough)[None, :]
    scaled = noise + signal * row_ramp[:, None] * col_ramp[None, :]
    return jnp.clip(scaled, -150.0, 150.0).astype(jnp.bfloat16)


def block_scale(own_key, shape, pieces, least, top_value):
    level, own = 1.0, jax.random.fold_in(own_key, 6)
    for axis_at, blocks in pieces:
        draws = jnp.exp(jax.random.uniform(jax.random.fold_in(own, axis_at), (blocks,), jnp.float32, least / len(pieces), top_value / len(pieces)))
        level = level * jnp.repeat(draws, shape[axis_at] // blocks).reshape([-1 if axis == axis_at else 1 for axis in range(len(shape))])
    return level


def centred(key, extent, scale, limit, shards=(), held_as=jnp.bfloat16):
    array = scale * jax.random.normal(key, extent, jnp.float32)
    if shards:
        array = array * block_scale(key, extent, shards, -0.22, 0.18)
    return jnp.clip(array, -limit, limit).astype(held_as)


def setup_inputs(seed: int = 0) -> dict:
    keys = jax.random.split(jax.random.key(seed), 4)
    return {
        "momentum": centred(keys[0], (ROWS, COLS), 1.0, 6.0, ((0, 4), (1, 8)), jnp.float32),
        "gradient": draw_gradient(jax.random.fold_in(keys[3], 71), 0),
        "q_basis": centred(keys[2], (COLS, RANK), COLS ** -0.5, 0.0390625, ((0, 8), (1, 4))),
    }


def reference(momentum, gradient, q_basis):
    buffer = momentum + gradient.astype(jnp.float32)
    buffer_low = buffer.astype(jnp.bfloat16)
    power = jnp.dot(buffer_low.astype(jnp.float32), q_basis.astype(jnp.float32), preferred_element_type=jnp.float32)
    gram = jnp.dot(power.T, power, precision=lax.Precision.HIGHEST)
    lower = jnp.linalg.cholesky(gram)
    p_basis = jax.scipy.linalg.solve_triangular(lower, power.T, lower=True).T
    p_low = p_basis.astype(jnp.bfloat16)
    right = jnp.dot(buffer_low.T.astype(jnp.float32), p_low.astype(jnp.float32), preferred_element_type=jnp.float32)
    sums = lax.optimization_barrier(jnp.sum(right * right, axis=0))
    q_next = right / jnp.sqrt(sums + 1e-06)
    right_low = right.astype(jnp.bfloat16)
    update = jnp.dot(p_low.astype(jnp.float32), right_low.T.astype(jnp.float32), preferred_element_type=jnp.float32)
    return (buffer - 0.1 * update, p_basis, q_next)
```

```python
import functools
import jax
import jax.numpy as jnp
from jax import lax
from jax.experimental import pallas as pl
from jax.experimental.pallas import tpu as pltpu
from jax.sharding import PartitionSpec as P

HI = lax.Precision.HIGHEST
SUB = 8


def mm(a, b, ca, cb):
    return lax.dot_general(a, b, (((ca,), (cb,)), ((), ())), precision=HI, preferred_element_type=jnp.float32)


def lanes(x, j, width):
    return jnp.broadcast_to(x[:, j:j + 1], (x.shape[0], width))


def subl(x, j):
    return jnp.broadcast_to(x[j:j + 1, :], x.shape)


def inverse_factor(left, n):
    blocks = n // SUB
    sub = lax.broadcasted_iota(jnp.int32, (SUB, n), 0)
    lane = lax.broadcasted_iota(jnp.int32, (SUB, n), 1)
    wl = [left[SUB * i:SUB * (i + 1), :] for i in range(blocks)]
    wr = [jnp.where(lane == sub + SUB * i, 1.0, 0.0).astype(jnp.float32) for i in range(blocks)]
    for p in range(blocks):
        cols = [lanes(wl[p], SUB * p + j, n) for j in range(SUB)]
        inv, rows_l, rows_r, fac = [], [], [], {}
        scale = jnp.zeros((SUB, n), jnp.float32)
        for j in range(SUB):
            d = subl(cols[j], j)
            r = 1.0 / d
            scale = jnp.where(sub == j, d, scale)
            m = jnp.where(sub > j, cols[j] * r, 0.0)
            inv.append(r)
            for k in range(j + 1, SUB):
                fac[j, k] = subl(cols[k], j)
                cols[k] = cols[k] - m * fac[j, k]
            rows_l.append(subl(wl[p], j))
            rows_r.append(subl(wr[p], j))
            wl[p] = wl[p] - m * rows_l[j]
            wr[p] = wr[p] - m * rows_r[j]
        wr[p] = wr[p] * lax.rsqrt(scale)
        for i in range(p + 1, blocks):
            c = [lanes(wl[i], SUB * p + j, n) for j in range(SUB)]
            for j in range(SUB):
                m = c[j] * inv[j]
                for k in range(j + 1, SUB):
                    c[k] = c[k] - m * fac[j, k]
                wl[i] = wl[i] - m * rows_l[j]
                wr[i] = wr[i] - m * rows_r[j]
    return jnp.concatenate(wr, axis=0)


def chol_kernel(nb, g_ref, x_ref, a_ref):
    rank = g_ref.shape[0]
    a_ref[...] = g_ref[...]
    rows = lax.broadcasted_iota(jnp.int32, (rank, rank), 0)
    cols = lax.broadcasted_iota(jnp.int32, (rank, rank), 1)
    x_ref[...] = jnp.where(rows == cols, 1.0, 0.0).astype(jnp.float32)
    row = lax.broadcasted_iota(jnp.int32, (rank, nb), 0)

    @pl.loop(0, rank // nb)
    def _(k):
        at = pl.ds(pl.multiple_of(k * nb, nb), nb)
        m = inverse_factor(a_ref[at, at], nb)
        low = jnp.where(row >= (k + 1) * nb, mm(a_ref[:, at], m, 1, 1), 0.0)
        xk = mm(m, x_ref[at, :], 1, 0)
        x_ref[at, :] = xk
        x_ref[...] -= mm(low, xk, 1, 0)
        a_ref[...] -= mm(low, low, 1, 1)


def chol_inverse(gram, nb=128):
    rank = gram.shape[0]
    return pl.pallas_call(
        functools.partial(chol_kernel, nb),
        out_shape=jax.ShapeDtypeStruct((rank, rank), jnp.float32),
        in_specs=[pl.BlockSpec(memory_space=pltpu.VMEM)],
        out_specs=pl.BlockSpec(memory_space=pltpu.VMEM),
        scratch_shapes=[pltpu.VMEM((rank, rank), jnp.float32)],
        cost_estimate=pl.CostEstimate(flops=30_000_000_000, bytes_accessed=8 * rank * rank, transcendentals=0),
        name="chol_inverse",
    )(gram)


def update_kernel(m_ref, g_ref, p_ref, r_ref, *rest):
    out_ref = rest[-1]
    product = lax.dot_general(
        p_ref[...], r_ref[...], (((1,), (1,)), ((), ())), preferred_element_type=jnp.float32
    )
    out_ref[...] = m_ref[...] + g_ref[...].astype(jnp.float32) - 0.1 * product


def update_piece(momentum, gradient, p_low, right_low, out, start, unit):
    rows, cols = momentum.shape
    width, rank = right_low.shape
    block = rows // 2 if rows % 16 == 0 else rows
    first = start // unit
    wide = pl.BlockSpec((block, unit), lambda j, i: (i, first + j))
    in_specs = [
        wide,
        wide,
        pl.BlockSpec((block, rank), lambda j, i: (i, 0)),
        pl.BlockSpec((unit, rank), lambda j, i: (j, 0)),
    ]
    args = [momentum, gradient, p_low, right_low]
    aliases = {}
    if out is not None:
        in_specs.append(pl.BlockSpec(memory_space=pl.ANY))
        args.append(out)
        aliases = {4: 0}
    return pl.pallas_call(
        update_kernel,
        grid=(width // unit, rows // block),
        out_shape=jax.ShapeDtypeStruct((rows, cols), jnp.float32),
        in_specs=in_specs,
        out_specs=wide,
        input_output_aliases=aliases,
        compiler_params=pltpu.CompilerParams(vmem_limit_bytes=40 * 1024 * 1024),
        cost_estimate=pl.CostEstimate(
            flops=2 * rows * width * rank, bytes_accessed=10 * rows * width, transcendentals=0
        ),
        name="update_piece",
    )(*args)


def exchange(x, axis, bit):
    n = lax.axis_size(axis)
    return lax.ppermute(x, axis, [(i, i ^ bit) for i in range(n)])


def bits_of(n):
    return [1 << b for b in range(n.bit_length() - 1)]


def scatter_sum(x, axis):
    n = lax.axis_size(axis)
    me = lax.axis_index(axis)
    v = x.reshape((n, x.shape[0] // n) + x.shape[1:])
    for bit in bits_of(n):
        b = (me // bit) % 2
        v = v.reshape((v.shape[0] // 2, 2) + v.shape[1:])
        keep = lax.dynamic_index_in_dim(v, b, 1, keepdims=False)
        send = lax.dynamic_index_in_dim(v, 1 - b, 1, keepdims=False)
        came = exchange(send, axis, bit)
        v = keep + came
    return v.reshape(v.shape[1:])


def gather(x, axis):
    n = lax.axis_size(axis)
    me = lax.axis_index(axis)
    v = x[None]
    for bit in reversed(bits_of(n)):
        b = (me // bit) % 2
        other = exchange(v, axis, bit)
        v = jnp.stack([jnp.where(b == 0, v, other), jnp.where(b == 0, other, v)], axis=1)
        v = v.reshape((v.shape[0] * 2,) + v.shape[2:])
    return v.reshape((v.shape[0] * v.shape[1],) + v.shape[2:])


def far_blocks(x, axis):
    n = lax.axis_size(axis)
    found = [x]
    for mask in range(2, n, 2):
        found.append(exchange(x, axis, mask))
    return jnp.concatenate(found, axis=0)


def near_gather(v, axis):
    me = lax.axis_index(axis)
    for bit in bits_of(v.shape[0]):
        b = (me // (2 * bit)) % 2
        w = v.reshape((-1, 2, bit) + v.shape[1:])
        w = jnp.stack([jnp.where(b == 0, w[:, 0], w[:, 1]), jnp.where(b == 0, w[:, 1], w[:, 0])], axis=1)
        v = w.reshape(v.shape)
    other = exchange(v, axis, 1)
    b = me % 2
    return jnp.stack([jnp.where(b == 0, v, other), jnp.where(b == 0, other, v)], axis=1)


def row_sum(x, axis):
    n = lax.axis_size(axis)
    total = x
    for d in range(1, n):
        total = total + lax.ppermute(x, axis, [(i, (i + d) % n) for i in range(n)])
    return total


def cuts_of(cols, pieces):
    unit = next((u for u in (256, 128) if cols % u == 0), cols)
    count = cols // unit
    n = min(pieces, count)
    return unit, [unit * ((count * k + n - 1) // n) for k in range(n + 1)]


PIECES = 7


def groups_of(nz):
    return [[0, 1]] + [[s] for s in range(2, nz)] if nz > 1 else [[0]]


def layer(momentum, gradient, q_basis):
    rows, cols = momentum.shape
    share = q_basis.shape[1]
    nz, nc = lax.axis_size("row"), lax.axis_size("col")
    z = lax.axis_index("row")
    rank = share * nz
    up = z < nz // 2

    to_right = [(i, i + 1) for i in range(nz - 1)]
    to_left = [(i + 1, i) for i in range(nz - 1)]
    from_left, from_right = [q_basis], [q_basis]
    for _ in range(1, nz):
        from_left.append(lax.ppermute(from_left[-1], "row", to_right))
        from_right.append(lax.ppermute(from_right[-1], "row", to_left))

    low = (momentum + gradient.astype(jnp.float32)).astype(jnp.bfloat16)
    low = lax.optimization_barrier(low)

    def chunk_of(s):
        if s == 0:
            return q_basis, z
        ahead, behind = from_right[s], from_left[s]
        if 2 * s > nz:
            ahead = jnp.where(z + s < nz, ahead, from_left[nz - s])
            behind = jnp.where(z >= s, behind, from_right[nz - s])
        chunk = jnp.where(up, ahead, behind)
        return chunk, jnp.where(up, z + s, z - s + nz) % nz

    block = jnp.zeros((rows // nc, rank), jnp.float32)
    for slots in groups_of(nz):
        chunks = [chunk_of(s) for s in slots]
        part = jnp.dot(
            low, jnp.concatenate([x for x, _ in chunks], 1), preferred_element_type=jnp.float32
        )
        whole = scatter_sum(part, "col")
        for k, (_, at) in enumerate(chunks):
            piece = whole[:, k * share:(k + 1) * share]
            block = lax.dynamic_update_slice_in_dim(block, piece, at * share, 1)

    local = lax.dot_general(block, block, (((0,), (0,)), ((), ())), precision=HI)
    gram = gather(row_sum(scatter_sum(local, "col"), "row"), "col")
    power = far_blocks(block, "col")
    inverse = chol_inverse(gram)
    turned = (((1,), (1,)), ((), ()))
    half = lax.dot_general(power, inverse, turned, precision=lax.Precision.HIGH)
    half = half.astype(jnp.bfloat16).reshape(-1, rows // nc, rank)
    p_low = near_gather(half, "col").reshape(rows, rank)
    p_out = lax.dot_general(block, inverse, turned, precision=HI)

    unit, cuts = cuts_of(cols, PIECES)
    out, own = None, []
    for start, stop in zip(cuts[:-1], cuts[1:]):
        part = jnp.einsum(
            "ic,ir->cr", low[:, start:stop], p_low, preferred_element_type=jnp.float32
        )
        came, total = None, part
        for h in range(1, nz):
            send = part if came is None else part + came.astype(jnp.float32)
            send = send.astype(jnp.bfloat16)
            came = lax.ppermute(send, "row", [(h - 1, h), (nz - h, nz - h - 1)])
            total = total + came.astype(jnp.float32)
        own.append(lax.dynamic_slice_in_dim(total, z * share, share, 1))
        out = update_piece(momentum, gradient, p_low, total.astype(jnp.bfloat16), out, start, unit)
    right = jnp.concatenate(own, axis=0)
    sums = jnp.sum(right * right, axis=0, keepdims=True)
    for bit in bits_of(nc):
        sums = sums + exchange(sums, "col", bit)
    q_next = right / jnp.sqrt(sums + 1e-06)
    return (out, p_out, q_next)


def solution(mesh):
    return jax.shard_map(
        layer,
        mesh=mesh,
        in_specs=(P("row", "col"), P("row", "col"), P("col", "row")),
        out_specs=(P("row", "col"), P(("row", "col"), None), P("col", "row")),
        check_vma=False,
    )
```
